32 devices in a mesh: gx: 2 (over x), gy: 4 (over z), gz: 4 (over y, core).
Axes of the slice: x: 2, y: 2, z: 4, core: 2. Of those that a mesh axis runs over, the one named last changes fastest.
Arguments:
- acts: bfloat16 [40960, 768], P(('gx', 'gy', 'gz')), may hold values from -6 to 6
- grads_out: bfloat16 [40960, 768], P(('gx', 'gy', 'gz')), may hold values from -0.03125 to 0.03125
- master: float32 [4608, 128], P(('gx', 'gy', 'gz')), may hold values from -0.3 to 0.3
- moment: float32 [4608, 128], P(('gx', 'gy', 'gz')), may hold values from -6 to 6
- second: float32 [4608, 128], P(('gx', 'gy', 'gz')), may hold values from 0.1 to 2
Outputs:
- master_new: float32 [4608, 128], P(('gx', 'gy', 'gz'))
- moment_new: float32 [4608, 128], P(('gx', 'gy', 'gz'))
- second_new: float32 [4608, 128], P(('gx', 'gy', 'gz'))
- weights: bfloat16 [768, 768], replicated
The draws below stay inside these ranges and needn't reach their ends.
All inputs are finite; a program needn't handle non-finite values.
Results may differ from the reference program's by a relative error of at most 0.003.
Values may be sent and summed in bfloat16 or wider, within the bound.
A program may use at most 64 MiB of HBM per device.

```python
import math
import jax
import jax.numpy as jnp
from jax import lax

IN = 768
OUT = 768
LANE = 128
STEP = 1000
TOK_DEV = 1280
TOKENS = 40960
FLAT = 4608


def spiked(result, own_key, source, target, shards_of, factor):
    def block_of(position):
        return (jnp.arange(result.shape[position]) // (result.shape[position] // shards_of)).reshape((-1,) + (1,) * (result.ndim - 1 - position))

    one_side = jax.random.permutation(own_key, shards_of)[block_of(target)]
    far = (block_of(target) + shards_of // 2) % shards_of
    return jnp.where((block_of(source) == one_side) | (block_of(source) == far), factor * result, result)


def block_levels(key, extent, cuts, least, top_value):
    gain, own = 1.0, jax.random.fold_in(key, 6)
    for dim, blocks in cuts:
        steps = jnp.exp(jax.random.uniform(jax.random.fold_in(own, dim), (blocks,), jnp.float32, least / len(cuts), top_value / len(cuts)))
        gain = gain * jnp.repeat(steps, extent[dim] // blocks).reshape([-1 if axis == dim else 1 for axis in range(len(extent))])
    return gain


def noise(own_key, shape, width, reach, shards=(), held_as=jnp.bfloat16):
    drawn = jax.random.normal(own_key, shape, jnp.float32) * width
    if len(shards) > 0:
        drawn = block_levels(own_key, shape, shards, -0.22, 0.18) * drawn
    return jnp.clip(drawn, min=-reach, max=reach).astype(held_as)


def gaussian_with(rng, shape, spread, reach, pieces, heavy, kind=jnp.bfloat16):
    array = spread * jax.random.normal(rng, shape, jnp.float32)
    if pieces:
        array = array * block_levels(rng, shape, pieces, -0.22, 0.18)
    return jnp.clip(spiked(array, jax.random.fold_in(rng, 3), *heavy), -reach, reach).astype(kind)


def setup_inputs(seed: int = 0) -> dict:
    keys = jax.random.split(jax.random.key(seed), 6)
    return {
        "acts": gaussian_with(keys[0], (TOKENS, IN), 1.0, 6.0, ((0, 32),), (0, 1, 32, 2.75)),
        "grads_out": noise(keys[1], (TOKENS, OUT), TOKENS ** -0.5, 0.03125, ((0, 32),)),
        "master": noise(keys[2], (FLAT, LANE), 0.05, 0.3, ((0, 32),), jnp.float32),
        "moment": noise(keys[3], (FLAT, LANE), 1.0, 6.0, ((0, 32),), jnp.float32),
        "second": jnp.clip(jnp.exp(math.log(2.0) - 2.9957323 * jax.random.uniform(keys[4], (FLAT, LANE), jnp.float32) ** block_levels(keys[4], (FLAT, LANE), ((0, 32),), -0.2, 0.2)), 0.1, 2.0),
    }


def reference(acts, grads_out, master, moment, second):
    blocks = TOKENS // TOK_DEV
    act_blocks = acts.reshape(blocks, TOK_DEV, IN)
    cot_blocks = grads_out.reshape(blocks, TOK_DEV, OUT)

    def add_block(total, pair):
        product = lax.dot_general(pair[0], pair[1], (((0,), (0,)), ((), ())), preferred_element_type=jnp.float32)
        return (total + product, None)
    start = jnp.zeros((IN, OUT), jnp.float32)
    gradient, _ = lax.scan(add_block, start, (act_blocks, cot_blocks))
    gradient = gradient.reshape(FLAT, LANE)
    moment_new = 0.9 * moment + 0.1 * gradient
    second_new = 0.95 * second + 0.05 * gradient * gradient
    first_fix = 1.0 - 0.9 ** STEP
    second_fix = 1.0 - 0.95 ** STEP
    ratio = moment_new / first_fix / (jnp.sqrt(second_new / second_fix) + 1e-08)
    master_new = master - 0.01 * (ratio + 0.01 * master)
    weights = master_new.astype(jnp.bfloat16).reshape(IN, OUT)
    return (master_new, moment_new, second_new, weights)
```

```python
import functools
import itertools

import jax
import jax.numpy as jnp
from jax import lax
from jax.experimental import pallas as pl
from jax.experimental.pallas import tpu as pltpu
from jax.sharding import PartitionSpec as P

STEP = 1000
MESH = pl.DeviceIdType.MESH
CORES = 2


def adam(gradient, master, moment, second):
    moment_new = 0.9 * moment + 0.1 * gradient
    second_new = 0.95 * second + 0.05 * gradient * gradient
    first_fix = 1.0 - 0.9**STEP
    second_fix = 1.0 - 0.95**STEP
    ratio = moment_new / first_fix / (jnp.sqrt(second_new / second_fix) + 1e-08)
    master_new = master - 0.01 * (ratio + 0.01 * master)
    return master_new, moment_new, second_new


def shards(acts, grads_out, master, moment, second):
    width_in = acts.shape[1]
    width_out = grads_out.shape[1]
    lane = master.shape[1]
    total_rows = width_in * width_out // lane
    local_grad = lax.dot_general(
        acts, grads_out, (((0,), (0,)), ((), ())), preferred_element_type=jnp.float32
    )
    value = local_grad.reshape(total_rows, lane)
    for axis in ("gx", "gy", "gz"):
        value = lax.psum_scatter(
            value.astype(jnp.bfloat16), axis, scatter_dimension=0, tiled=True
        ).astype(jnp.float32)
    master_new, moment_new, second_new = adam(value, master, moment, second)
    gathered = master_new.astype(jnp.bfloat16)
    for axis in ("gz", "gy", "gx"):
        gathered = lax.all_gather(gathered, axis, axis=0, tiled=True)
    weights = gathered.reshape(width_in, width_out)
    return (master_new, moment_new, second_new, weights)


def flip(value, bits):
    bit = 1
    while bit <= bits:
        if bits & bit:
            value = value + bit - 2 * bit * (lax.rem(value // bit, 2))
        bit *= 2
    return value


def kernel(
    nx, nz, ny,
    acts_ref, grads_ref, master_ref, moment_ref, second_ref,
    master_out, moment_out, second_out, weights_out,
    part, pair_out, pair_in, out, inn, full,
    pair_send, pair_recv, link_send, link_recv,
    gather_send, gather_recv, twin_send, twin_recv,
):
    x = lax.axis_index("gx")
    z = lax.axis_index("gy")
    g = lax.axis_index("gz")
    y = g // CORES
    core = lax.rem(g, CORES)
    lane = master_ref.shape[1]
    rows = acts_ref.shape[1] // (nx * nz * ny * CORES)
    strips = grads_ref.shape[1] // lane
    block_rows = rows * strips

    def peer(kx=0, kz=0, ky=0, kc=0):
        return (flip(x, kx), flip(z, kz), flip(y, ky) * CORES + flip(core, kc))

    def owner(kx, kz, ky, kc):
        px, pz, pg = peer(kx, kz, ky, kc)
        return (px * nz + pz) * (ny * CORES) + pg

    def slot(kx, kz, ky):
        return (kx * nz + kz) * ny + ky

    xs, zs, ys = range(1, nx), range(1, nz), range(1, ny)
    peers = [peer(kc=1)] + [peer(kx=k) for k in xs]
    peers += [peer(ky=k) for k in ys] + [peer(kz=k) for k in zs]

    barrier = pltpu.get_barrier_semaphore()
    for target in peers:
        pl.semaphore_signal(barrier, inc=1, device_id=target, device_id_type=MESH)

    part[...] = lax.dot_general(
        acts_ref[...], grads_ref[...], (((0,), (0,)), ((), ())),
        preferred_element_type=jnp.float32,
    )

    def mine(kx, kz, ky, kc):
        top = pl.multiple_of(owner(kx, kz, ky, kc) * rows, 8)
        return jnp.concatenate(
            [part[pl.ds(top, rows), s * lane:(s + 1) * lane] for s in range(strips)], axis=0
        )

    def x_first(kz):
        return kz % 2 == 0

    first, second_step, third = [], [], []
    for kz in reversed(range(nz)):
        for ky, kx in itertools.product(reversed(range(ny)), reversed(range(nx))):
            if (kx if x_first(kz) else ky) != 0:
                first.append((kx, kz, ky))
            elif (ky if x_first(kz) else kx) != 0:
                second_step.append((kx, kz, ky))
            else:
                third.append((kx, kz, ky))
    first.sort(key=lambda k: -(k[0] != 0) - (k[2] != 0))

    pl.semaphore_wait(barrier, len(peers))

    started = []

    def send(src, dst, send_sem, recv_sem, target):
        copy = pltpu.make_async_remote_copy(
            src_ref=src, dst_ref=dst, send_sem=send_sem, recv_sem=recv_sem,
            device_id=target, device_id_type=MESH,
        )
        copy.start()
        started.append(copy)

    def arrived(dst, send_sem, recv_sem):
        pltpu.make_async_remote_copy(
            src_ref=dst, dst_ref=dst, send_sem=send_sem, recv_sem=recv_sem,
            device_id=peer(kc=1), device_id_type=MESH,
        ).wait_recv()

    for k in first + second_step + third:
        i = slot(*k)
        pair_out[i] = mine(*k, 1).astype(jnp.bfloat16)
        send(pair_out.at[i], pair_in.at[i], pair_send.at[i], pair_recv.at[i], peer(kc=1))

    def take(i):
        arrived(inn.at[i], link_send.at[i], link_recv.at[i])
        return inn[i].astype(jnp.float32)

    def total(k):
        kx, kz, ky = k
        i = slot(*k)
        arrived(pair_in.at[i], pair_send.at[i], pair_recv.at[i])
        value = mine(*k, 0) + pair_in[i].astype(jnp.float32)
        if x_first(kz):
            if kx == 0:
                for p in xs:
                    value += take(slot(p, kz, ky))
                if ky == 0:
                    for p in ys:
                        value += take(slot(0, kz, p))
        else:
            if ky == 0:
                for p in ys:
                    value += take(slot(kx, kz, p))
                if kx == 0:
                    for p in xs:
                        value += take(slot(p, kz, 0))
        return value

    def pass_on(k, target):
        i = slot(*k)
        out[i] = total(k).astype(jnp.bfloat16)
        send(out.at[i], inn.at[i], link_send.at[i], link_recv.at[i], target)

    for k in first:
        kx, kz, ky = k
        pass_on(k, peer(kx=kx) if x_first(kz) else peer(ky=ky))
    for k in second_step:
        kx, kz, ky = k
        pass_on(k, peer(ky=ky) if x_first(kz) else peer(kx=kx))
    gradient = None
    for k in third:
        if k[1] != 0:
            pass_on(k, peer(kz=k[1]))
        else:
            gradient = total(k)
    for kz in zs:
        gradient += take(slot(0, kz, 0))

    me = owner(0, 0, 0, 0)
    updated = []
    for s in range(strips):
        at = pl.ds(s, rows, stride=strips)
        master_new, moment_new, second_new = adam(
            gradient[s * rows:(s + 1) * rows],
            master_ref[at, :], moment_ref[at, :], second_ref[at, :],
        )
        master_out[at, :] = master_new
        moment_out[at, :] = moment_new
        second_out[at, :] = second_new
        updated.append(master_new)
    full[me] = jnp.concatenate(updated, axis=0).astype(jnp.bfloat16)

    def forward(k, kx, kz, ky):
        i = slot(kx, kz, ky)
        here = full.at[owner(*k, 0)]
        target = peer(kx=kx ^ k[0], kz=kz ^ k[1], ky=ky ^ k[2])
        send(here, here, gather_send.at[i], gather_recv.at[i], target)

    def twin(k):
        i = slot(*k)
        here = full.at[owner(*k, 0)]
        send(here, here, twin_send.at[i], twin_recv.at[i], peer(kc=1))

    def receive(k):
        i = slot(*k)
        arrived(full.at[owner(*k, 0)], gather_send.at[i], gather_recv.at[i])

    def spread(k):
        kx, kz, ky = k
        if kx == 0 and ky == 0 and kz == 0:
            for p in reversed(zs):
                forward(k, 0, p, 0)
        if x_first(kz):
            if kx == 0 and ky == 0:
                for p in ys:
                    forward(k, 0, kz, p)
            if kx == 0:
                for p in xs:
                    forward(k, p, kz, ky)
        else:
            if kx == 0 and ky == 0:
                for p in xs:
                    forward(k, p, kz, 0)
            if ky == 0:
                for p in ys:
                    forward(k, kx, kz, p)
        twin(k)

    def middle(kz):
        if x_first(kz):
            return [(0, kz, p) for p in ys]
        return [(p, kz, 0) for p in xs]

    def last(kz):
        if x_first(kz):
            return [(p, kz, q) for q in range(ny) for p in xs]
        return [(p, kz, q) for p in range(nx) for q in ys]

    order = [(0, 0, 0)] + middle(0)
    for kz in zs:
        order += [(0, kz, 0)] + (last(kz - 1) if kz == 1 else middle(kz - 1))
    order += middle(nz - 1)
    for kz in zs:
        order += last(kz)
    seen = []
    for k in order:
        if k in seen:
            continue
        seen.append(k)
        if k != (0, 0, 0):
            receive(k)
        spread(k)

    chip_rows = CORES * rows
    for k in seen:
        i = slot(*k)
        arrived(full.at[owner(*k, 1)], twin_send.at[i], twin_recv.at[i])
        pair = owner(*k, 0) // CORES
        top = pl.multiple_of(pair * chip_rows, 16)
        low = full[pair * CORES].astype(jnp.float32)
        high = full[pair * CORES + 1].astype(jnp.float32)
        for s in range(strips):
            both = jnp.concatenate(
                [low[s * rows:(s + 1) * rows], high[s * rows:(s + 1) * rows]], axis=0
            )
            weights_out[pl.ds(top, chip_rows), s * lane:(s + 1) * lane] = both.astype(jnp.bfloat16)

    for copy in started:
        copy.wait_send()


def fused(nx, nz, ny, acts, grads_out, master, moment, second):
    width_in, width_out = acts.shape[1], grads_out.shape[1]
    flat, lane = master.shape
    chips = nx * nz * ny
    block = (flat, lane)
    vmem = pl.BlockSpec(memory_space=pltpu.VMEM)
    sems = pltpu.SemaphoreType.DMA((chips,))
    return pl.pallas_call(
        functools.partial(kernel, nx, nz, ny),
        out_shape=(
            jax.ShapeDtypeStruct(block, jnp.float32),
            jax.ShapeDtypeStruct(block, jnp.float32),
            jax.ShapeDtypeStruct(block, jnp.float32),
            jax.ShapeDtypeStruct((width_in, width_out), jnp.bfloat16),
        ),
        in_specs=[vmem] * 5,
        out_specs=(vmem,) * 4,
        scratch_shapes=[
            pltpu.VMEM((width_in, width_out), jnp.float32),
            pltpu.VMEM((chips,) + block, jnp.bfloat16),
            pltpu.VMEM((chips,) + block, jnp.bfloat16),
            pltpu.VMEM((chips,) + block, jnp.bfloat16),
            pltpu.VMEM((chips,) + block, jnp.bfloat16),
            pltpu.VMEM((chips * CORES,) + block, jnp.bfloat16),
        ] + [sems] * 8,
        compiler_params=pltpu.CompilerParams(collective_id=0, has_side_effects=True),
    )(acts, grads_out, master, moment, second)


def power_of_two(n):
    return n & (n - 1) == 0


def body(mesh, acts, grads_out, master, moment, second):
    nx, nz, ng = mesh.shape["gx"], mesh.shape["gy"], mesh.shape["gz"]
    devices = nx * nz * ng
    whole_rows = acts.shape[1] % (8 * devices) == 0 and grads_out.shape[1] % master.shape[1] == 0
    even = (grads_out.shape[1] // master.shape[1]) % 2 == 0
    if whole_rows and even and ng % CORES == 0 and all(map(power_of_two, (nx, nz, ng))):
        return fused(nx, nz, ng // CORES, acts, grads_out, master, moment, second)
    return shards(acts, grads_out, master, moment, second)


def solution(mesh):
    split = P(("gx", "gy", "gz"), None)
    return jax.shard_map(
        functools.partial(body, mesh),
        mesh=mesh,
        in_specs=(split,) * 5,
        out_specs=(split, split, split, P()),
        check_vma=False,
    )
```

```python
import functools
import itertools

import jax
import jax.numpy as jnp
from jax import lax
from jax.experimental import pallas as pl
from jax.experimental.pallas import tpu as pltpu
from jax.sharding import PartitionSpec as P

STEP = 1000
MESH = pl.DeviceIdType.MESH
CORES = 2


def adam(gradient, master, moment, second):
    moment_new = 0.9 * moment + 0.1 * gradient
    second_new = 0.95 * second + 0.05 * gradient * gradient
    first_fix = 1.0 - 0.9**STEP
    second_fix = 1.0 - 0.95**STEP
    ratio = moment_new / first_fix / (jnp.sqrt(second_new / second_fix) + 1e-08)
    master_new = master - 0.01 * (ratio + 0.01 * master)
    return master_new, moment_new, second_new


def shards(acts, grads_out, master, moment, second):
    width_in = acts.shape[1]
    width_out = grads_out.shape[1]
    lane = master.shape[1]
    total_rows = width_in * width_out // lane
    local_grad = lax.dot_general(
        acts, grads_out, (((0,), (0,)), ((), ())), preferred_element_type=jnp.float32
    )
    value = local_grad.reshape(total_rows, lane)
    for axis in ("gx", "gy", "gz"):
        value = lax.psum_scatter(
            value.astype(jnp.bfloat16), axis, scatter_dimension=0, tiled=True
        ).astype(jnp.float32)
    master_new, moment_new, second_new = adam(value, master, moment, second)
    gathered = master_new.astype(jnp.bfloat16)
    for axis in ("gz", "gy", "gx"):
        gathered = lax.all_gather(gathered, axis, axis=0, tiled=True)
    weights = gathered.reshape(width_in, width_out)
    return (master_new, moment_new, second_new, weights)


def flip(value, bits):
    bit = 1
    while bit <= bits:
        if bits & bit:
            value = value + bit - 2 * bit * (lax.rem(value // bit, 2))
        bit *= 2
    return value


def kernel(
    nx, nz, ny,
    acts_ref, grads_ref, master_hbm, moment_hbm, second_hbm,
    master_out, moment_out, second_out, full,
    acts_in, grads_in, master_ref, moment_ref, second_ref, part, pair_out, pair_in, out, inn,
    load, pair_send, pair_recv, link_send, link_recv,
    gather_send, gather_recv, twin_send, twin_recv,
):
    x = lax.axis_index("gx")
    z = lax.axis_index("gy")
    g = lax.axis_index("gz")
    y = g // CORES
    core = lax.rem(g, CORES)
    lane = master_ref.shape[1]
    rows = acts_ref.shape[1] // (nx * nz * ny * CORES)
    strips = grads_ref.shape[1] // lane
    block_rows = rows * strips

    def peer(kx=0, kz=0, ky=0, kc=0):
        return (flip(x, kx), flip(z, kz), flip(y, ky) * CORES + flip(core, kc))

    def owner(kx, kz, ky, kc):
        px, pz, pg = peer(kx, kz, ky, kc)
        return (px * nz + pz) * (ny * CORES) + pg

    def slot(kx, kz, ky):
        return (kx * nz + kz) * ny + ky

    xs, zs, ys = range(1, nx), range(1, nz), range(1, ny)
    peers = [peer(kc=1)] + [peer(kx=k) for k in xs]
    peers += [peer(ky=k) for k in ys] + [peer(kz=k) for k in zs]

    barrier = pltpu.get_barrier_semaphore()
    for target in peers:
        pl.semaphore_signal(barrier, inc=1, device_id=target, device_id_type=MESH)

    width = acts_ref.shape[1] // nx

    def columns(kx):
        return pl.ds(pl.multiple_of(flip(x, kx) * width, lane), width)

    loads = [pltpu.make_async_copy(grads_ref, grads_in, load.at[nx])]
    for kx in reversed(range(nx)):
        loads.append(
            pltpu.make_async_copy(acts_ref.at[:, columns(kx)], acts_in.at[kx], load.at[kx])
        )
    state = ((master_hbm, master_ref), (moment_hbm, moment_ref), (second_hbm, second_ref))
    for i, (src, dst) in enumerate(state):
        loads.append(pltpu.make_async_copy(src, dst, load.at[nx + 1 + i]))
    for copy in loads:
        copy.start()

    def mine(kx, kz, ky, kc):
        top = pl.multiple_of(owner(kx, kz, ky, kc) * rows, 8)
        return jnp.concatenate(
            [part[pl.ds(top, rows), s * lane:(s + 1) * lane] for s in range(strips)], axis=0
        )

    def x_first(kz):
        return kz % 2 == 0

    first, second_step, third = [], [], []
    for kz in reversed(range(nz)):
        for ky, kx in itertools.product(reversed(range(ny)), reversed(range(nx))):
            if (kx if x_first(kz) else ky) != 0:
                first.append((kx, kz, ky))
            elif (ky if x_first(kz) else kx) != 0:
                second_step.append((kx, kz, ky))
            else:
                third.append((kx, kz, ky))
    first.sort(key=lambda k: -(k[0] != 0) - (k[2] != 0))

    started = []

    def send(src, dst, send_sem, recv_sem, target):
        copy = pltpu.make_async_remote_copy(
            src_ref=src, dst_ref=dst, send_sem=send_sem, recv_sem=recv_sem,
            device_id=target, device_id_type=MESH,
        )
        copy.start()
        started.append(copy)

    def arrived(dst, send_sem, recv_sem):
        pltpu.make_async_remote_copy(
            src_ref=dst, dst_ref=dst, send_sem=send_sem, recv_sem=recv_sem,
            device_id=peer(kc=1), device_id_type=MESH,
        ).wait_recv()

    loads[0].wait()
    for kx in reversed(range(nx)):
        loads[nx - kx].wait()
        part[columns(kx), :] = lax.dot_general(
            acts_in[kx], grads_in[...], (((0,), (0,)), ((), ())),
            preferred_element_type=jnp.float32,
        )
        if kx == nx - 1:
            pl.semaphore_wait(barrier, len(peers))
        for k in first + second_step + third:
            if k[0] == kx:
                i = slot(*k)
                pair_out[i] = mine(*k, 1).astype(jnp.bfloat16)
                send(pair_out.at[i], pair_in.at[i], pair_send.at[i], pair_recv.at[i], peer(kc=1))

    def take(i):
        arrived(inn.at[i], link_send.at[i], link_recv.at[i])
        return inn[i].astype(jnp.float32)

    def total(k):
        kx, kz, ky = k
        i = slot(*k)
        arrived(pair_in.at[i], pair_send.at[i], pair_recv.at[i])
        value = mine(*k, 0) + pair_in[i].astype(jnp.float32)
        if x_first(kz):
            if kx == 0:
                for p in xs:
                    value += take(slot(p, kz, ky))
                if ky == 0:
                    for p in ys:
                        value += take(slot(0, kz, p))
        else:
            if ky == 0:
                for p in ys:
                    value += take(slot(kx, kz, p))
                if kx == 0:
                    for p in xs:
                        value += take(slot(p, kz, 0))
        return value

    def pass_on(k, target):
        i = slot(*k)
        out[i] = total(k).astype(jnp.bfloat16)
        send(out.at[i], inn.at[i], link_send.at[i], link_recv.at[i], target)

    for k in first:
        kx, kz, ky = k
        pass_on(k, peer(kx=kx) if x_first(kz) else peer(ky=ky))
    for k in second_step:
        kx, kz, ky = k
        pass_on(k, peer(ky=ky) if x_first(kz) else peer(kx=kx))
    gradient = None
    for k in third:
        if k[1] != 0:
            pass_on(k, peer(kz=k[1]))
        else:
            gradient = total(k)
    for kz in zs:
        gradient += take(slot(0, kz, 0))

    for copy in loads[nx + 1:]:
        copy.wait()
    me = owner(0, 0, 0, 0)
    updated = []
    for s in range(strips):
        at = pl.ds(s, rows, stride=strips)
        master_new, moment_new, second_new = adam(
            gradient[s * rows:(s + 1) * rows],
            master_ref[at, :], moment_ref[at, :], second_ref[at, :],
        )
        master_out[at, :] = master_new
        moment_out[at, :] = moment_new
        second_out[at, :] = second_new
        updated.append(master_new)
    full[me] = jnp.concatenate(updated, axis=0).astype(jnp.bfloat16)

    def forward(k, kx, kz, ky):
        i = slot(kx, kz, ky)
        here = full.at[owner(*k, 0)]
        target = peer(kx=kx ^ k[0], kz=kz ^ k[1], ky=ky ^ k[2])
        send(here, here, gather_send.at[i], gather_recv.at[i], target)

    def twin(k):
        i = slot(*k)
        here = full.at[owner(*k, 0)]
        send(here, here, twin_send.at[i], twin_recv.at[i], peer(kc=1))

    def receive(k):
        i = slot(*k)
        arrived(full.at[owner(*k, 0)], gather_send.at[i], gather_recv.at[i])

    def spread(k):
        kx, kz, ky = k
        if kx == 0 and ky == 0 and kz == 0:
            for p in reversed(zs):
                forward(k, 0, p, 0)
        if x_first(kz):
            if kx == 0 and ky == 0:
                for p in ys:
                    forward(k, 0, kz, p)
            if kx == 0:
                for p in xs:
                    forward(k, p, kz, ky)
        else:
            if kx == 0 and ky == 0:
                for p in xs:
                    forward(k, p, kz, 0)
            if ky == 0:
                for p in ys:
                    forward(k, kx, kz, p)
        twin(k)

    def middle(kz):
        if x_first(kz):
            return [(0, kz, p) for p in ys]
        return [(p, kz, 0) for p in xs]

    def last(kz):
        if x_first(kz):
            return [(p, kz, q) for q in range(ny) for p in xs]
        return [(p, kz, q) for p in range(nx) for q in ys]

    order = [(0, 0, 0)] + middle(0)
    for kz in zs:
        order += [(0, kz, 0)] + (last(kz - 1) if kz == 1 else middle(kz - 1))
    order += middle(nz - 1)
    for kz in zs:
        order += last(kz)
    seen = []
    for k in order:
        if k in seen:
            continue
        seen.append(k)
        if k != (0, 0, 0):
            receive(k)
        spread(k)

    for k in seen:
        i = slot(*k)
        arrived(full.at[owner(*k, 1)], twin_send.at[i], twin_recv.at[i])

    for copy in started:
        copy.wait_send()


def finish(
    master_ref, moment_ref, second_ref, full,
    master_out, moment_out, second_out, weights_out,
    weights, store,
):
    blocks, _, lane = full.shape
    rows = weights.shape[0] // blocks
    strips = weights.shape[1] // lane
    pairs = blocks // CORES
    copies = []
    plain = ((master_ref, master_out), (moment_ref, moment_out), (second_ref, second_out))
    for i, (src, dst) in enumerate(plain):
        copies.append(pltpu.make_async_copy(src, dst, store.at[i]))
        copies[-1].start()
    groups = 4 if pairs % 4 == 0 else 1
    chip_rows = CORES * rows
    for group in range(groups):
        for pair in range(group * pairs // groups, (group + 1) * pairs // groups):
            low = full[pair * CORES].astype(jnp.float32)
            high = full[pair * CORES + 1].astype(jnp.float32)
            for s in range(strips):
                both = jnp.concatenate(
                    [low[s * rows:(s + 1) * rows], high[s * rows:(s + 1) * rows]], axis=0
                )
                weights[pair * chip_rows:(pair + 1) * chip_rows, s * lane:(s + 1) * lane] = (
                    both.astype(jnp.bfloat16)
                )
        span = pl.ds(group * (weights.shape[0] // groups), weights.shape[0] // groups)
        copies.append(
            pltpu.make_async_copy(weights.at[span, :], weights_out.at[span, :], store.at[3 + group])
        )
        copies[-1].start()
    for copy in copies:
        copy.wait()


VMEM_BYTES = 67_043_328
LIMIT = 24 * 1024 * 1024


def fused(nx, nz, ny, acts, grads_out, master, moment, second):
    tokens, width_in = acts.shape
    width_out = grads_out.shape[1]
    block = master.shape
    chips = nx * nz * ny
    vmem = pl.BlockSpec(memory_space=pltpu.VMEM)
    hbm = pl.BlockSpec(memory_space=pl.ANY)
    sems = pltpu.SemaphoreType.DMA((chips,))
    kept = 2 * width_in * width_out + 3 * 4 * master.size
    limit = (VMEM_BYTES - kept - 32 * 1024) // 1024 * 1024
    results = pl.pallas_call(
        functools.partial(kernel, nx, nz, ny),
        out_shape=(
            pltpu.VMEM(block, jnp.float32),
            pltpu.VMEM(block, jnp.float32),
            pltpu.VMEM(block, jnp.float32),
            pltpu.VMEM((chips * CORES,) + block, jnp.bfloat16),
        ),
        in_specs=[pl.BlockSpec(memory_space=pltpu.HBM)] * 5,
        out_specs=(vmem,) * 4,
        scratch_shapes=[
            pltpu.VMEM((nx, tokens, width_in // nx), jnp.bfloat16),
            pltpu.VMEM((tokens, width_out), jnp.bfloat16),
            pltpu.VMEM(block, jnp.float32),
            pltpu.VMEM(block, jnp.float32),
            pltpu.VMEM(block, jnp.float32),
            pltpu.VMEM((width_in, width_out), jnp.float32),
            pltpu.VMEM((chips,) + block, jnp.bfloat16),
            pltpu.VMEM((chips,) + block, jnp.bfloat16),
            pltpu.VMEM((chips,) + block, jnp.bfloat16),
            pltpu.VMEM((chips,) + block, jnp.bfloat16),
            pltpu.SemaphoreType.DMA((nx + 4,)),
        ] + [sems] * 8,
        compiler_params=pltpu.CompilerParams(
            collective_id=0, has_side_effects=True, vmem_limit_bytes=limit
        ),
    )(acts, grads_out, master, moment, second)
    return pl.pallas_call(
        finish,
        out_shape=(
            jax.ShapeDtypeStruct(block, jnp.float32),
            jax.ShapeDtypeStruct(block, jnp.float32),
            jax.ShapeDtypeStruct(block, jnp.float32),
            jax.ShapeDtypeStruct((width_in, width_out), jnp.bfloat16),
        ),
        in_specs=[vmem] * 4,
        out_specs=(hbm,) * 4,
        scratch_shapes=[
            pltpu.VMEM((width_in, width_out), jnp.bfloat16),
            pltpu.SemaphoreType.DMA((7,)),
        ],
        compiler_params=pltpu.CompilerParams(vmem_limit_bytes=LIMIT),
    )(*results)


def power_of_two(n):
    return n & (n - 1) == 0


def body(mesh, acts, grads_out, master, moment, second):
    nx, nz, ng = mesh.shape["gx"], mesh.shape["gy"], mesh.shape["gz"]
    devices = nx * nz * ng
    whole_rows = acts.shape[1] % (8 * devices) == 0 and grads_out.shape[1] % master.shape[1] == 0
    whole_rows = whole_rows and acts.shape[1] % (nx * master.shape[1]) == 0
    even = (grads_out.shape[1] // master.shape[1]) % 2 == 0
    if whole_rows and even and ng % CORES == 0 and all(map(power_of_two, (nx, nz, ng))):
        return fused(nx, nz, ng // CORES, acts, grads_out, master, moment, second)
    return shards(acts, grads_out, master, moment, second)


def solution(mesh):
    split = P(("gx", "gy", "gz"), None)
    return jax.shard_map(
        functools.partial(body, mesh),
        mesh=mesh,
        in_specs=(split,) * 5,
        out_specs=(split, split, split, P()),
        check_vma=False,
    )
```

```python
import functools
import itertools

import jax
import jax.numpy as jnp
from jax import lax
from jax.experimental import pallas as pl
from jax.experimental.pallas import tpu as pltpu
from jax.sharding import PartitionSpec as P

STEP = 1000
MESH = pl.DeviceIdType.MESH
CORES = 2


def adam(gradient, master, moment, second):
    moment_new = 0.9 * moment + 0.1 * gradient
    second_new = 0.95 * second + 0.05 * gradient * gradient
    first_fix = 1.0 - 0.9**STEP
    second_fix = 1.0 - 0.95**STEP
    ratio = moment_new / first_fix / (jnp.sqrt(second_new / second_fix) + 1e-08)
    master_new = master - 0.01 * (ratio + 0.01 * master)
    return master_new, moment_new, second_new


def shards(acts, grads_out, master, moment, second):
    width_in = acts.shape[1]
    width_out = grads_out.shape[1]
    lane = master.shape[1]
    total_rows = width_in * width_out // lane
    local_grad = lax.dot_general(
        acts, grads_out, (((0,), (0,)), ((), ())), preferred_element_type=jnp.float32
    )
    value = local_grad.reshape(total_rows, lane)
    for axis in ("gx", "gy", "gz"):
        value = lax.psum_scatter(
            value.astype(jnp.bfloat16), axis, scatter_dimension=0, tiled=True
        ).astype(jnp.float32)
    master_new, moment_new, second_new = adam(value, master, moment, second)
    gathered = master_new.astype(jnp.bfloat16)
    for axis in ("gz", "gy", "gx"):
        gathered = lax.all_gather(gathered, axis, axis=0, tiled=True)
    weights = gathered.reshape(width_in, width_out)
    return (master_new, moment_new, second_new, weights)


def flip(value, bits):
    bit = 1
    while bit <= bits:
        if bits & bit:
            value = value + bit - 2 * bit * (lax.rem(value // bit, 2))
        bit *= 2
    return value


def kernel(
    nx, nz, ny,
    acts_ref, grads_ref, master_hbm, moment_hbm, second_hbm,
    master_out, moment_out, second_out, full,
    acts_in, grads_in, master_ref, moment_ref, second_ref, part, pair_out, pair_in, out, inn,
    load, pair_send, pair_recv, link_send, link_recv,
    gather_send, gather_recv, twin_send, twin_recv,
):
    x = lax.axis_index("gx")
    z = lax.axis_index("gy")
    g = lax.axis_index("gz")
    y = g // CORES
    core = lax.rem(g, CORES)
    lane = master_ref.shape[1]
    rows = acts_ref.shape[1] // (nx * nz * ny * CORES)
    strips = grads_ref.shape[1] // lane
    block_rows = rows * strips

    def peer(kx=0, kz=0, ky=0, kc=0):
        return (flip(x, kx), flip(z, kz), flip(y, ky) * CORES + flip(core, kc))

    def owner(kx, kz, ky, kc):
        px, pz, pg = peer(kx, kz, ky, kc)
        return (px * nz + pz) * (ny * CORES) + pg

    def slot(kx, kz, ky):
        return (kx * nz + kz) * ny + ky

    xs, zs, ys = range(1, nx), range(1, nz), range(1, ny)
    plane = [(p, q) for p in reversed(range(nx)) for q in reversed(range(ny)) if p + q]
    peers = [peer(kc=1)] + [peer(kx=p, ky=q) for p, q in plane] + [peer(kz=k) for k in zs]

    barrier = pltpu.get_barrier_semaphore()
    for target in peers:
        pl.semaphore_signal(barrier, inc=1, device_id=target, device_id_type=MESH)

    width = acts_ref.shape[1] // nx

    def columns(kx):
        return pl.ds(pl.multiple_of(flip(x, kx) * width, lane), width)

    loads = [pltpu.make_async_copy(grads_ref, grads_in, load.at[nx])]
    for kx in reversed(range(nx)):
        loads.append(
            pltpu.make_async_copy(acts_ref.at[:, columns(kx)], acts_in.at[kx], load.at[kx])
        )
    state = ((master_hbm, master_ref), (moment_hbm, moment_ref), (second_hbm, second_ref))
    for i, (src, dst) in enumerate(state):
        loads.append(pltpu.make_async_copy(src, dst, load.at[nx + 1 + i]))
    for copy in loads:
        copy.start()

    def mine(kx, kz, ky, kc):
        top = pl.multiple_of(owner(kx, kz, ky, kc) * rows, 8)
        return jnp.concatenate(
            [part[pl.ds(top, rows), s * lane:(s + 1) * lane] for s in range(strips)], axis=0
        )

    def at_once(kz):
        return kz == nz - 1 and nz > 1

    def x_first(kz):
        return kz % 2 == 0

    first, second_step, third = [], [], []
    for kz in reversed(range(nz)):
        for ky, kx in itertools.product(reversed(range(ny)), reversed(range(nx))):
            if (kx if x_first(kz) else ky) != 0 or (at_once(kz) and kx + ky):
                first.append((kx, kz, ky))
            elif (ky if x_first(kz) else kx) != 0:
                second_step.append((kx, kz, ky))
            else:
                third.append((kx, kz, ky))
    first.sort(key=lambda k: -(k[0] != 0) - (k[2] != 0))

    started = []

    def send(src, dst, send_sem, recv_sem, target):
        copy = pltpu.make_async_remote_copy(
            src_ref=src, dst_ref=dst, send_sem=send_sem, recv_sem=recv_sem,
            device_id=target, device_id_type=MESH,
        )
        copy.start()
        started.append(copy)

    def arrived(dst, send_sem, recv_sem):
        pltpu.make_async_remote_copy(
            src_ref=dst, dst_ref=dst, send_sem=send_sem, recv_sem=recv_sem,
            device_id=peer(kc=1), device_id_type=MESH,
        ).wait_recv()

    def take(i):
        arrived(inn.at[i], link_send.at[i], link_recv.at[i])
        return inn[i].astype(jnp.float32)

    def total(k):
        kx, kz, ky = k
        i = slot(*k)
        arrived(pair_in.at[i], pair_send.at[i], pair_recv.at[i])
        value = mine(*k, 0) + pair_in[i].astype(jnp.float32)
        if at_once(kz):
            if kx == 0 and ky == 0:
                for p, q in plane:
                    value += take(slot(p, kz, q))
        elif x_first(kz):
            if kx == 0:
                for p in xs:
                    value += take(slot(p, kz, ky))
                if ky == 0:
                    for p in ys:
                        value += take(slot(0, kz, p))
        else:
            if ky == 0:
                for p in ys:
                    value += take(slot(kx, kz, p))
                if kx == 0:
                    for p in xs:
                        value += take(slot(p, kz, 0))
        return value

    def pass_on(k, target):
        i = slot(*k)
        out[i] = total(k).astype(jnp.bfloat16)
        send(out.at[i], inn.at[i], link_send.at[i], link_recv.at[i], target)

    def first_step(k):
        kx, kz, ky = k
        if at_once(kz):
            pass_on(k, peer(kx=kx, ky=ky))
        else:
            pass_on(k, peer(kx=kx) if x_first(kz) else peer(ky=ky))

    loads[0].wait()
    for kx in reversed(range(nx)):
        loads[nx - kx].wait()
        halves = 2 if kx == 0 else 1
        for half in range(halves):
            wide = pl.ds(half * (strips * lane // halves), strips * lane // halves)
            part[columns(kx), wide] = lax.dot_general(
                acts_in[kx], grads_in[:, wide], (((0,), (0,)), ((), ())),
                preferred_element_type=jnp.float32,
            )
            if kx == 0 and half == 0:
                for k in first:
                    if k[0] != 0:
                        first_step(k)
        if kx == nx - 1:
            pl.semaphore_wait(barrier, len(peers))
        for k in first + second_step + third:
            if k[0] == kx:
                i = slot(*k)
                pair_out[i] = mine(*k, 1).astype(jnp.bfloat16)
                send(pair_out.at[i], pair_in.at[i], pair_send.at[i], pair_recv.at[i], peer(kc=1))

    for k in first:
        if k[0] == 0:
            first_step(k)
    gradient = None
    for k in second_step + third:
        kx, kz, ky = k
        if k == (0, 0, 0):
            gradient = total(k)
        elif k in third:
            pass_on(k, peer(kz=kz))
        else:
            pass_on(k, peer(ky=ky) if x_first(kz) else peer(kx=kx))
    for kz in zs:
        gradient += take(slot(0, kz, 0))

    for copy in loads[nx + 1:]:
        copy.wait()
    me = owner(0, 0, 0, 0)
    updated = []
    for s in range(strips):
        at = pl.ds(s, rows, stride=strips)
        master_new, moment_new, second_new = adam(
            gradient[s * rows:(s + 1) * rows],
            master_ref[at, :], moment_ref[at, :], second_ref[at, :],
        )
        master_out[at, :] = master_new
        moment_out[at, :] = moment_new
        second_out[at, :] = second_new
        updated.append(master_new)
    full[me] = jnp.concatenate(updated, axis=0).astype(jnp.bfloat16)

    def forward(k, kx, kz, ky):
        i = slot(kx, kz, ky)
        here = full.at[owner(*k, 0)]
        target = peer(kx=kx ^ k[0], kz=kz ^ k[1], ky=ky ^ k[2])
        send(here, here, gather_send.at[i], gather_recv.at[i], target)

    def twin(k):
        i = slot(*k)
        here = full.at[owner(*k, 0)]
        send(here, here, twin_send.at[i], twin_recv.at[i], peer(kc=1))

    def receive(k):
        i = slot(*k)
        arrived(full.at[owner(*k, 0)], gather_send.at[i], gather_recv.at[i])

    def spread(k):
        kx, kz, ky = k
        if kx == 0 and ky == 0 and kz == 0:
            for p in zs:
                forward(k, 0, p, 0)
        if kx == 0 and ky == 0:
            for p, q in plane:
                forward(k, p, kz, q)
        twin(k)

    order = [(0, kz, 0) for kz in range(nz)]
    order += [(p, kz, q) for kz in range(nz) for p, q in reversed(plane)]
    for k in order:
        if k != (0, 0, 0):
            receive(k)
        spread(k)

    for k in order:
        i = slot(*k)
        arrived(full.at[owner(*k, 1)], twin_send.at[i], twin_recv.at[i])

    for copy in started:
        copy.wait_send()


def finish(
    master_ref, moment_ref, second_ref, full,
    master_out, moment_out, second_out, weights_out,
    weights, store,
):
    blocks, _, lane = full.shape
    rows = weights.shape[0] // blocks
    strips = weights.shape[1] // lane
    pairs = blocks // CORES
    copies = []
    plain = ((master_ref, master_out), (moment_ref, moment_out), (second_ref, second_out))
    for i, (src, dst) in enumerate(plain):
        copies.append(pltpu.make_async_copy(src, dst, store.at[i]))
        copies[-1].start()
    groups = 4 if pairs % 4 == 0 else 1
    chip_rows = CORES * rows
    for group in range(groups):
        for pair in range(group * pairs // groups, (group + 1) * pairs // groups):
            low = full[pair * CORES].astype(jnp.float32)
            high = full[pair * CORES + 1].astype(jnp.float32)
            for s in range(strips):
                both = jnp.concatenate(
                    [low[s * rows:(s + 1) * rows], high[s * rows:(s + 1) * rows]], axis=0
                )
                weights[pair * chip_rows:(pair + 1) * chip_rows, s * lane:(s + 1) * lane] = (
                    both.astype(jnp.bfloat16)
                )
        span = pl.ds(group * (weights.shape[0] // groups), weights.shape[0] // groups)
        copies.append(
            pltpu.make_async_copy(weights.at[span, :], weights_out.at[span, :], store.at[3 + group])
        )
        copies[-1].start()
    for copy in copies:
        copy.wait()


VMEM_BYTES = 67_043_328
LIMIT = 24 * 1024 * 1024


def fused(nx, nz, ny, acts, grads_out, master, moment, second):
    tokens, width_in = acts.shape
    width_out = grads_out.shape[1]
    block = master.shape
    chips = nx * nz * ny
    vmem = pl.BlockSpec(memory_space=pltpu.VMEM)
    hbm = pl.BlockSpec(memory_space=pl.ANY)
    sems = pltpu.SemaphoreType.DMA((chips,))
    kept = 2 * width_in * width_out + 3 * 4 * master.size
    limit = (VMEM_BYTES - kept - 32 * 1024) // 1024 * 1024
    results = pl.pallas_call(
        functools.partial(kernel, nx, nz, ny),
        out_shape=(
            pltpu.VMEM(block, jnp.float32),
            pltpu.VMEM(block, jnp.float32),
            pltpu.VMEM(block, jnp.float32),
            pltpu.VMEM((chips * CORES,) + block, jnp.bfloat16),
        ),
        in_specs=[pl.BlockSpec(memory_space=pltpu.HBM)] * 5,
        out_specs=(vmem,) * 4,
        scratch_shapes=[
            pltpu.VMEM((nx, tokens, width_in // nx), jnp.bfloat16),
            pltpu.VMEM((tokens, width_out), jnp.bfloat16),
            pltpu.VMEM(block, jnp.float32),
            pltpu.VMEM(block, jnp.float32),
            pltpu.VMEM(block, jnp.float32),
            pltpu.VMEM((width_in, width_out), jnp.float32),
            pltpu.VMEM((chips,) + block, jnp.bfloat16),
            pltpu.VMEM((chips,) + block, jnp.bfloat16),
            pltpu.VMEM((chips,) + block, jnp.bfloat16),
            pltpu.VMEM((chips,) + block, jnp.bfloat16),
            pltpu.SemaphoreType.DMA((nx + 4,)),
        ] + [sems] * 8,
        compiler_params=pltpu.CompilerParams(
            collective_id=0, has_side_effects=True, vmem_limit_bytes=limit
        ),
    )(acts, grads_out, master, moment, second)
    return pl.pallas_call(
        finish,
        out_shape=(
            jax.ShapeDtypeStruct(block, jnp.float32),
            jax.ShapeDtypeStruct(block, jnp.float32),
            jax.ShapeDtypeStruct(block, jnp.float32),
            jax.ShapeDtypeStruct((width_in, width_out), jnp.bfloat16),
        ),
        in_specs=[vmem] * 4,
        out_specs=(hbm,) * 4,
        scratch_shapes=[
            pltpu.VMEM((width_in, width_out), jnp.bfloat16),
            pltpu.SemaphoreType.DMA((7,)),
        ],
        compiler_params=pltpu.CompilerParams(vmem_limit_bytes=LIMIT),
    )(*results)


def power_of_two(n):
    return n & (n - 1) == 0


def body(mesh, acts, grads_out, master, moment, second):
    nx, nz, ng = mesh.shape["gx"], mesh.shape["gy"], mesh.shape["gz"]
    devices = nx * nz * ng
    whole_rows = acts.shape[1] % (8 * devices) == 0 and grads_out.shape[1] % master.shape[1] == 0
    whole_rows = whole_rows and acts.shape[1] % (nx * master.shape[1]) == 0
    even = (grads_out.shape[1] // master.shape[1]) % 2 == 0
    if whole_rows and even and ng % CORES == 0 and all(map(power_of_two, (nx, nz, ng))):
        return fused(nx, nz, ng // CORES, acts, grads_out, master, moment, second)
    return shards(acts, grads_out, master, moment, second)


def solution(mesh):
    split = P(("gx", "gy", "gz"), None)
    return jax.shard_map(
        functools.partial(body, mesh),
        mesh=mesh,
        in_specs=(split,) * 5,
        out_specs=(split, split, split, P()),
        check_vma=False,
    )
```

```python
import functools
import itertools

import jax
import jax.numpy as jnp
from jax import lax
from jax.experimental import pallas as pl
from jax.experimental.pallas import tpu as pltpu
from jax.sharding import PartitionSpec as P

STEP = 1000
MESH = pl.DeviceIdType.MESH
CORES = 2


def adam(gradient, master, moment, second):
    moment_new = 0.9 * moment + 0.1 * gradient
    second_new = 0.95 * second + 0.05 * gradient * gradient
    first_fix = 1.0 - 0.9**STEP
    second_fix = 1.0 - 0.95**STEP
    ratio = moment_new / first_fix / (jnp.sqrt(second_new / second_fix) + 1e-08)
    master_new = master - 0.01 * (ratio + 0.01 * master)
    return master_new, moment_new, second_new


def shards(acts, grads_out, master, moment, second):
    width_in = acts.shape[1]
    width_out = grads_out.shape[1]
    lane = master.shape[1]
    total_rows = width_in * width_out // lane
    local_grad = lax.dot_general(
        acts, grads_out, (((0,), (0,)), ((), ())), preferred_element_type=jnp.float32
    )
    value = local_grad.reshape(total_rows, lane)
    for axis in ("gx", "gy", "gz"):
        value = lax.psum_scatter(
            value.astype(jnp.bfloat16), axis, scatter_dimension=0, tiled=True
        ).astype(jnp.float32)
    master_new, moment_new, second_new = adam(value, master, moment, second)
    gathered = master_new.astype(jnp.bfloat16)
    for axis in ("gz", "gy", "gx"):
        gathered = lax.all_gather(gathered, axis, axis=0, tiled=True)
    weights = gathered.reshape(width_in, width_out)
    return (master_new, moment_new, second_new, weights)


def flip(value, bits):
    bit = 1
    while bit <= bits:
        if bits & bit:
            value = value + bit - 2 * bit * (lax.rem(value // bit, 2))
        bit *= 2
    return value


def kernel(
    nx, nz, ny,
    acts_ref, grads_ref, master_hbm, moment_hbm, second_hbm,
    master_out, moment_out, second_out, weights,
    acts_in, grads_in, master_ref, moment_ref, second_ref, part, pair_out, pair_in, out, inn, full,
    load, pair_send, pair_recv, link_send, link_recv,
    gather_send, gather_recv, twin_send, twin_recv,
):
    x = lax.axis_index("gx")
    z = lax.axis_index("gy")
    g = lax.axis_index("gz")
    y = g // CORES
    core = lax.rem(g, CORES)
    lane = master_ref.shape[1]
    rows = acts_ref.shape[1] // (nx * nz * ny * CORES)
    strips = grads_ref.shape[1] // lane
    block_rows = rows * strips

    def peer(kx=0, kz=0, ky=0, kc=0):
        return (flip(x, kx), flip(z, kz), flip(y, ky) * CORES + flip(core, kc))

    def owner(kx, kz, ky, kc):
        px, pz, pg = peer(kx, kz, ky, kc)
        return (px * nz + pz) * (ny * CORES) + pg

    def slot(kx, kz, ky):
        return (kx * nz + kz) * ny + ky

    xs, zs, ys = range(1, nx), range(1, nz), range(1, ny)
    plane = [(p, q) for p in reversed(range(nx)) for q in reversed(range(ny)) if p + q]
    peers = [peer(kc=1)] + [peer(kx=p, ky=q) for p, q in plane] + [peer(kz=k) for k in zs]

    barrier = pltpu.get_barrier_semaphore()
    for target in peers:
        pl.semaphore_signal(barrier, inc=1, device_id=target, device_id_type=MESH)

    width = acts_ref.shape[1] // nx

    def columns(kx):
        return pl.ds(pl.multiple_of(flip(x, kx) * width, lane), width)

    loads = [pltpu.make_async_copy(grads_ref, grads_in, load.at[nx])]
    for kx in reversed(range(nx)):
        loads.append(
            pltpu.make_async_copy(acts_ref.at[:, columns(kx)], acts_in.at[kx], load.at[kx])
        )
    state = ((master_hbm, master_ref), (moment_hbm, moment_ref), (second_hbm, second_ref))
    for i, (src, dst) in enumerate(state):
        loads.append(pltpu.make_async_copy(src, dst, load.at[nx + 1 + i]))
    for copy in loads:
        copy.start()

    def mine(kx, kz, ky, kc):
        top = pl.multiple_of(owner(kx, kz, ky, kc) * rows, 8)
        return jnp.concatenate(
            [part[pl.ds(top, rows), s * lane:(s + 1) * lane] for s in range(strips)], axis=0
        )

    def at_once(kz):
        return kz == nz - 1 and nz > 1

    def x_first(kz):
        return kz % 2 == 0

    first, second_step, third = [], [], []
    for kz in reversed(range(nz)):
        for ky, kx in itertools.product(reversed(range(ny)), reversed(range(nx))):
            if (kx if x_first(kz) else ky) != 0 or (at_once(kz) and kx + ky):
                first.append((kx, kz, ky))
            elif (ky if x_first(kz) else kx) != 0:
                second_step.append((kx, kz, ky))
            else:
                third.append((kx, kz, ky))
    first.sort(key=lambda k: -(k[0] != 0) - (k[2] != 0))

    started = []

    def send(src, dst, send_sem, recv_sem, target):
        copy = pltpu.make_async_remote_copy(
            src_ref=src, dst_ref=dst, send_sem=send_sem, recv_sem=recv_sem,
            device_id=target, device_id_type=MESH,
        )
        copy.start()
        started.append(copy)

    def arrived(dst, send_sem, recv_sem):
        pltpu.make_async_remote_copy(
            src_ref=dst, dst_ref=dst, send_sem=send_sem, recv_sem=recv_sem,
            device_id=peer(kc=1), device_id_type=MESH,
        ).wait_recv()

    def take(i):
        arrived(inn.at[i], link_send.at[i], link_recv.at[i])
        return inn[i].astype(jnp.float32)

    def total(k):
        kx, kz, ky = k
        i = slot(*k)
        arrived(pair_in.at[i], pair_send.at[i], pair_recv.at[i])
        value = mine(*k, 0) + pair_in[i].astype(jnp.float32)
        if at_once(kz):
            if kx == 0 and ky == 0:
                for p, q in plane:
                    value += take(slot(p, kz, q))
        elif x_first(kz):
            if kx == 0:
                for p in xs:
                    value += take(slot(p, kz, ky))
                if ky == 0:
                    for p in ys:
                        value += take(slot(0, kz, p))
        else:
            if ky == 0:
                for p in ys:
                    value += take(slot(kx, kz, p))
                if kx == 0:
                    for p in xs:
                        value += take(slot(p, kz, 0))
        return value

    def pass_on(k, target):
        i = slot(*k)
        out[i] = total(k).astype(jnp.bfloat16)
        send(out.at[i], inn.at[i], link_send.at[i], link_recv.at[i], target)

    def first_step(k):
        kx, kz, ky = k
        if at_once(kz):
            pass_on(k, peer(kx=kx, ky=ky))
        else:
            pass_on(k, peer(kx=kx) if x_first(kz) else peer(ky=ky))

    loads[0].wait()
    for kx in reversed(range(nx)):
        loads[nx - kx].wait()
        halves = 2 if kx == 0 else 1
        for half in range(halves):
            wide = pl.ds(half * (strips * lane // halves), strips * lane // halves)
            part[columns(kx), wide] = lax.dot_general(
                acts_in[kx], grads_in[:, wide], (((0,), (0,)), ((), ())),
                preferred_element_type=jnp.float32,
            )
            if kx == 0 and half == 0:
                for k in first:
                    if k[0] != 0:
                        first_step(k)
        if kx == nx - 1:
            pl.semaphore_wait(barrier, len(peers))
        for k in first + second_step + third:
            if k[0] == kx:
                i = slot(*k)
                pair_out[i] = mine(*k, 1).astype(jnp.bfloat16)
                send(pair_out.at[i], pair_in.at[i], pair_send.at[i], pair_recv.at[i], peer(kc=1))

    for k in first:
        if k[0] == 0:
            first_step(k)
    gradient = None
    for k in second_step + third:
        kx, kz, ky = k
        if k == (0, 0, 0):
            gradient = total(k)
        elif k in third:
            pass_on(k, peer(kz=kz))
        else:
            pass_on(k, peer(ky=ky) if x_first(kz) else peer(kx=kx))
    for kz in zs:
        gradient += take(slot(0, kz, 0))

    for copy in loads[nx + 1:]:
        copy.wait()
    me = owner(0, 0, 0, 0)
    updated = []
    for s in range(strips):
        at = pl.ds(s, rows, stride=strips)
        master_new, moment_new, second_new = adam(
            gradient[s * rows:(s + 1) * rows],
            master_ref[at, :], moment_ref[at, :], second_ref[at, :],
        )
        master_out[at, :] = master_new
        moment_out[at, :] = moment_new
        second_out[at, :] = second_new
        updated.append(master_new)
    full[me] = jnp.concatenate(updated, axis=0).astype(jnp.bfloat16)

    def forward(k, kx, kz, ky):
        i = slot(kx, kz, ky)
        here = full.at[owner(*k, 0)]
        target = peer(kx=kx ^ k[0], kz=kz ^ k[1], ky=ky ^ k[2])
        send(here, here, gather_send.at[i], gather_recv.at[i], target)

    def twin(k):
        i = slot(*k)
        here = full.at[owner(*k, 0)]
        send(here, here, twin_send.at[i], twin_recv.at[i], peer(kc=1))

    def receive(k):
        i = slot(*k)
        arrived(full.at[owner(*k, 0)], gather_send.at[i], gather_recv.at[i])

    def spread(k):
        kx, kz, ky = k
        if kx == 0 and ky == 0 and kz == 0:
            for p in zs:
                forward(k, 0, p, 0)
        if kx == 0 and ky == 0:
            for p, q in plane:
                forward(k, p, kz, q)
        twin(k)

    order = [(0, kz, 0) for kz in range(nz)]
    order += [(p, kz, q) for kz in range(nz) for p, q in reversed(plane)]
    for k in order:
        if k != (0, 0, 0):
            receive(k)
        spread(k)

    chip_rows = CORES * rows
    for k in order:
        i = slot(*k)
        arrived(full.at[owner(*k, 1)], twin_send.at[i], twin_recv.at[i])
        pair = owner(*k, 0) // CORES
        top = pl.ds(pl.multiple_of(pair * chip_rows, chip_rows), chip_rows)
        low = full[pair * CORES].astype(jnp.float32)
        high = full[pair * CORES + 1].astype(jnp.float32)
        for s in range(strips):
            span = slice(s * rows, (s + 1) * rows)
            both = jnp.concatenate([low[span], high[span]], axis=0)
            weights[top, s * lane:(s + 1) * lane] = both.astype(jnp.bfloat16)

    for copy in started:
        copy.wait_send()


def finish(*refs):
    store = refs[-1]
    half = (len(refs) - 1) // 2
    copies = [
        pltpu.make_async_copy(src, dst, store.at[i])
        for i, (src, dst) in enumerate(zip(refs[:half], refs[half:-1]))
    ]
    for copy in reversed(copies):
        copy.start()
    for copy in copies:
        copy.wait()


VMEM_BYTES = 67_043_328
LIMIT = 24 * 1024 * 1024


def fused(nx, nz, ny, acts, grads_out, master, moment, second):
    tokens, width_in = acts.shape
    width_out = grads_out.shape[1]
    block = master.shape
    chips = nx * nz * ny
    vmem = pl.BlockSpec(memory_space=pltpu.VMEM)
    hbm = pl.BlockSpec(memory_space=pl.ANY)
    sems = pltpu.SemaphoreType.DMA((chips,))
    kept = 2 * width_in * width_out + 3 * 4 * master.size
    limit = (VMEM_BYTES - kept - 32 * 1024) // 1024 * 1024
    results = pl.pallas_call(
        functools.partial(kernel, nx, nz, ny),
        out_shape=(
            pltpu.VMEM(block, jnp.float32),
            pltpu.VMEM(block, jnp.float32),
            pltpu.VMEM(block, jnp.float32),
            pltpu.VMEM((width_in, width_out), jnp.bfloat16),
        ),
        in_specs=[pl.BlockSpec(memory_space=pltpu.HBM)] * 5,
        out_specs=(vmem,) * 4,
        scratch_shapes=[
            pltpu.VMEM((nx, tokens, width_in // nx), jnp.bfloat16),
            pltpu.VMEM((tokens, width_out), jnp.bfloat16),
            pltpu.VMEM(block, jnp.float32),
            pltpu.VMEM(block, jnp.float32),
            pltpu.VMEM(block, jnp.float32),
            pltpu.VMEM((width_in, width_out), jnp.float32),
            pltpu.VMEM((chips,) + block, jnp.bfloat16),
            pltpu.VMEM((chips,) + block, jnp.bfloat16),
            pltpu.VMEM((chips,) + block, jnp.bfloat16),
            pltpu.VMEM((chips,) + block, jnp.bfloat16),
            pltpu.VMEM((chips * CORES,) + block, jnp.bfloat16),
            pltpu.SemaphoreType.DMA((nx + 5,)),
        ] + [sems] * 8,
        compiler_params=pltpu.CompilerParams(
            collective_id=0, has_side_effects=True, vmem_limit_bytes=limit
        ),
    )(acts, grads_out, master, moment, second)
    return pl.pallas_call(
        finish,
        out_shape=(
            jax.ShapeDtypeStruct(block, jnp.float32),
            jax.ShapeDtypeStruct(block, jnp.float32),
            jax.ShapeDtypeStruct(block, jnp.float32),
            jax.ShapeDtypeStruct((width_in, width_out), jnp.bfloat16),
        ),
        in_specs=[vmem] * 4,
        out_specs=(hbm,) * 4,
        scratch_shapes=[
            pltpu.SemaphoreType.DMA((4,)),
        ],
        compiler_params=pltpu.CompilerParams(vmem_limit_bytes=LIMIT),
    )(*results)


def power_of_two(n):
    return n & (n - 1) == 0


def body(mesh, acts, grads_out, master, moment, second):
    nx, nz, ng = mesh.shape["gx"], mesh.shape["gy"], mesh.shape["gz"]
    devices = nx * nz * ng
    whole_rows = acts.shape[1] % (8 * devices) == 0 and grads_out.shape[1] % master.shape[1] == 0
    whole_rows = whole_rows and acts.shape[1] % (nx * master.shape[1]) == 0
    even = (grads_out.shape[1] // master.shape[1]) % 2 == 0
    if whole_rows and even and ng % CORES == 0 and all(map(power_of_two, (nx, nz, ng))):
        return fused(nx, nz, ng // CORES, acts, grads_out, master, moment, second)
    return shards(acts, grads_out, master, moment, second)


def solution(mesh):
    split = P(("gx", "gy", "gz"), None)
    return jax.shard_map(
        functools.partial(body, mesh),
        mesh=mesh,
        in_specs=(split,) * 5,
        out_specs=(split, split, split, P()),
        check_vma=False,
    )
```
